256 devices in a mesh: tm: 4 (over y_hi, core), anta: 32 (over x, z), antb: 2 (over y_lo).
Axes of the slice: x: 4, y: 4 (y_hi: 2, y_lo: 2; y = y_hi * 2 + y_lo), z: 8, core: 2. Of those that a mesh axis runs over, the one named last changes fastest.
Arguments:
- samples: bfloat16 [2, 512, 6144], P('antb', 'anta', 'tm'), may hold values from -6 to 6
Outputs:
- correlation: float32 [256, 2, 512, 2, 512], P('tm', None, 'anta', 'antb')
The draws below stay inside these ranges and needn't reach their ends.
All inputs are finite; a program needn't handle non-finite values.
Results may differ from the reference program's by a relative error of at most 0.0003.
Values may be sent and summed in bfloat16 or wider, within the bound.
A program may use at most 64 MiB of HBM per device.

```python
import math
import jax
import jax.numpy as jnp
from jax import lax

ANTENNA_COUNT = 512
POLARISATION_NUM = 2
LAG_TOTAL = 256
TIME = 6144


def block_levels(rng, extent, pieces, smallest, largest):
    gain, own = 1.0, jax.random.fold_in(rng, 6)
    for position, blocks in pieces:
        steps = jnp.exp(jax.random.uniform(jax.random.fold_in(own, position), (blocks,), jnp.float32, smallest / len(pieces), largest / len(pieces)))
        gain = gain * jnp.repeat(steps, extent[position] // blocks).reshape([-1 if axis == position else 1 for axis in range(len(extent))])
    return gain


def centred(own_key, shape, spread, most, cuts=(), kind=jnp.bfloat16):
    array = spread * jax.random.normal(own_key, shape, jnp.float32)
    if cuts:
        array = array * block_levels(own_key, shape, cuts, -0.22, 0.18)
    return jnp.clip(array, -most, most).astype(kind)


def setup_inputs(seed: int = 0) -> dict:
    key_of = jax.random.split(jax.random.key(seed), 2)
    samples = centred(key_of[0], (POLARISATION_NUM, ANTENNA_COUNT, TIME), 1.0, 6.0, ((0, 2), (1, 32), (2, 4)))
    return dict(samples=samples)


def reference(samples):
    flat_samples = samples.reshape(POLARISATION_NUM * ANTENNA_COUNT, TIME)
    padded = jnp.pad(flat_samples, ((0, 0), (0, LAG_TOTAL)))

    def one_lag(lag_index):
        shifted = lax.dynamic_slice_in_dim(padded, lag_index, TIME, 1)
        return jnp.dot(flat_samples, shifted.T, preferred_element_type=jnp.float32)
    lagged = lax.map(one_lag, jnp.arange(LAG_TOTAL, dtype=jnp.int32))
    return (lagged * (1.0 / math.sqrt(TIME))).reshape(LAG_TOTAL, POLARISATION_NUM, ANTENNA_COUNT, POLARISATION_NUM, ANTENNA_COUNT)
```

```python
import functools
import math

import jax
import jax.numpy as jnp
from jax import lax
from jax.experimental import pallas as pl
from jax.experimental.pallas import tpu as pltpu
from jax.sharding import PartitionSpec as P

LAGS = 256
POLS = 2
ROWS = 16
BLOCK = 1536
PHASES = 12
TIMES = 4
NX, NZ, NY = 4, 8, 4
PORTION = 64
TABLE = PORTION + PHASES - 1
WHOLE = (0, 1536)
PART_P = (0, 896)
PART_Q = (896, 1536)
HALF = {
    WHOLE: {1: (0, 768), -1: (768, 1536)},
    PART_P: {1: (0, 512), -1: (512, 896)},
    PART_Q: {1: (896, 1152), -1: (1152, 1536)},
}
DZS = (0, 1, -1, 2, -2, 3, -3, 4)


def kernel_body(x_ref, acc, gathered, rows, table, xt, send_sem, recv_sem):
    tm = lax.axis_index("tm")
    anta = lax.axis_index("anta")
    antb = lax.axis_index("antb")
    y_hi, core = tm // 2, tm % 2
    x, z = anta // NZ, anta % NZ
    y = y_hi * 2 + antb
    tm_partner = y_hi * 2 + (1 - core)
    tm_other = (1 - y_hi) * 2 + core
    tm_last = (1 - y_hi) * 2 + (1 - core)

    def wrap(value, size):
        return lax.rem(value + size, size)

    x_next = {s: wrap(x + s, NX) * NZ + z for s in (1, -1)}
    z_next = {s: x * NZ + wrap(z + s, NZ) for s in (1, -1)}
    z_row = {dz: wrap(z + dz, NZ) * ROWS for dz in range(-4, 5)}

    def at_x(s):
        return {"tm": tm, "anta": x_next[s], "antb": antb}

    def at_z(s):
        return {"tm": tm, "anta": z_next[s], "antb": antb}

    def at_y(s):
        there = wrap(y + s, NY)
        return {"tm": (there // 2) * 2 + core, "anta": anta, "antb": there % 2}

    partner = {"tm": tm_partner, "anta": anta, "antb": antb}
    opposite = {"tm": tm_other, "anta": anta, "antb": antb}

    counter = {}

    def slot(key):
        return counter.setdefault(key, len(counter))

    sent = []

    def copy_of(key, src, dst, device):
        n = slot(key)
        return pltpu.make_async_remote_copy(
            src_ref=src, dst_ref=dst, send_sem=send_sem.at[n], recv_sem=recv_sem.at[n],
            device_id=device, device_id_type=pl.DeviceIdType.MESH,
        )

    def send(key, src, dst, device):
        copy = copy_of(key, src, dst, device)
        copy.start()
        sent.append(copy)

    def wait(key, dst):
        copy_of(key, dst, dst, partner).wait_recv()

    def block(time, rx, dz, lanes):
        row = pl.multiple_of((rx % NX) * (NZ * ROWS) + z_row[dz], ROWS)
        return gathered.at[time, pl.ds(row, ROWS), pl.ds(lanes[0], lanes[1] - lanes[0])]

    def row_block(time, pol):
        return rows.at[time + 1, pl.ds(pl.multiple_of(pol * ROWS, ROWS), ROWS), :]

    def send_z(g, time, s, rx, d):
        lanes = WHOLE if rx == 0 else PART_Q
        if d == 4:
            lanes = HALF[lanes][s]
        ref = block(time, rx, -s * (d - 1), lanes)
        send((g, "z", s, rx, d), ref, ref, at_z(s))

    def send_x(g, time, s, dz, d):
        lanes = WHOLE if dz == 0 else PART_P
        if d == 2:
            lanes = HALF[lanes][s]
        src = block(time, -s * (d - 1), dz, lanes)
        dst = block(time, -s * d, dz, lanes)
        send((g, "x", s, dz, d), src, dst, at_x(s))

    def wait_z(g, time, s, rx, d):
        lanes = WHOLE if rx == 0 else PART_Q
        if d == 4:
            lanes = HALF[lanes][s]
        wait((g, "z", s, rx, d), block(time, rx, -s * d, lanes))

    def wait_x(g, time, s, dz, d):
        lanes = WHOLE if dz == 0 else PART_P
        if d == 2:
            lanes = HALF[lanes][s]
        wait((g, "x", s, dz, d), block(time, -s * d, dz, lanes))

    def start(g, time):
        for s in (1, -1):
            send_z(g, time, s, 0, 1)
        for s in (1, -1):
            send_x(g, time, s, 0, 1)

    def level(g, time, n):
        for rx in (0, 1, 3, 2):
            d = n - {0: 0, 1: 1, 3: 1, 2: 2}[rx]
            if not 1 <= d <= 4:
                continue
            for s in (1, -1):
                wait_z(g, time, s, rx, d)
                if d < 4:
                    send_z(g, time, s, rx, d + 1)
                if rx == 0 and d < 4:
                    for sx in (1, -1):
                        send_x(g, time, sx, -s * d, 1)
            if rx == 0 and d == 4:
                for sx in (1, -1):
                    send_x(g, time, sx, 4, 1)
        for dz in DZS:
            d = n - abs(dz)
            if not 1 <= d <= 2:
                continue
            for s in (1, -1):
                wait_x(g, time, s, dz, d)
                if d == 1:
                    send_x(g, time, s, dz, 2)
                    if dz == 0:
                        for sz in (1, -1):
                            send_z(g, time, sz, -s % NX, 1)
            if dz == 0 and d == 2:
                for sz in (1, -1):
                    send_z(g, time, sz, 2, 1)
        done = {4: (0,), 5: (1, 3), 6: (2,)}.get(n, ())
        for rx in done:
            ref = gathered.at[time, pl.ds(rx * NZ * ROWS, NZ * ROWS), :]
            send((g, "plane", rx), ref, ref, partner)

    def planes(g, time):
        for rx in range(NX):
            wait((g, "plane", rx), gathered.at[time, pl.ds(rx * NZ * ROWS, NZ * ROWS), :])

    barrier = pltpu.get_barrier_semaphore()
    everyone = [at_x(1), at_x(-1), at_z(1), at_z(-1), at_y(1), at_y(-1), opposite, partner]
    for device in everyone:
        pl.semaphore_signal(barrier, inc=1, device_id=device, device_id_type=pl.DeviceIdType.MESH)

    own = x_ref[...].astype(jnp.float32)
    pad = jnp.zeros((128 - ROWS, 128), jnp.float32)
    for tile in range(PHASES):
        piece = jnp.concatenate([own[:, tile * 128:(tile + 1) * 128], pad], 0)
        xt[tile * 128:(tile + 1) * 128, :] = piece.T
    own_row = pl.multiple_of(z * ROWS, ROWS)
    pol_row = pl.multiple_of(antb * ROWS, ROWS)
    for phase in range(PHASES):
        piece = xt[pl.ds(phase, 128, stride=PHASES), :].T[:ROWS, :].astype(jnp.bfloat16)
        lanes = slice(phase * 128, (phase + 1) * 128)
        gathered[tm, pl.ds(own_row, ROWS), lanes] = piece
        rows[tm + 1, pl.ds(pol_row, ROWS), lanes] = piece
    rows[0, :, :] = jnp.zeros((POLS * ROWS, BLOCK), jnp.bfloat16)

    pl.semaphore_wait(barrier, len(everyone))

    own_block = block(tm, 0, 0, WHOLE)
    send("y2", own_block, own_block, opposite)
    start(0, tm)
    for s in (1, -1):
        send(("y", s), own_block, row_block(tm, antb), at_y(s))
    send("own", own_block, row_block(tm, antb), partner)

    level(0, tm, 1)
    wait("y2", block(tm_other, 0, 0, WHOLE))
    start(1, tm_other)
    other_block = block(tm_other, 0, 0, WHOLE)
    send("other", other_block, row_block(tm_other, antb), partner)
    for s in (1, -1):
        there = wrap(y - s, NY)
        ref = row_block((there // 2) * 2 + core, 1 - antb)
        wait(("y", s), ref)
        send(("row", s), ref, ref, partner)
    level(0, tm, 2)
    wait("own", row_block(tm_partner, antb))
    wait("other", row_block(tm_last, antb))
    for s in (1, -1):
        there = wrap(y - s, NY)
        wait(("row", s), row_block((there // 2) * 2 + 1 - core, 1 - antb))
    rows[tm_other + 1, pl.ds(pol_row, ROWS), :] = gathered[tm_other, pl.ds(own_row, ROWS), :]
    level(0, tm, 3)
    level(1, tm_other, 1)

    lane = lax.broadcasted_iota(jnp.int32, (POLS * ROWS, 128), 1)

    def build(n, carry):
        m = PHASES - 1 - n - PORTION * tm + PHASES * 32
        phase, shift = m % PHASES, 32 - m // PHASES
        lanes = pl.ds(pl.multiple_of(phase * 128, 128), 128)
        keep = lane >= shift
        to = pl.ds(pl.multiple_of(n * POLS * ROWS, POLS * ROWS), POLS * ROWS)
        before = pltpu.roll(rows[0, :, lanes], shift, 1)
        for time in range(TIMES):
            now = pltpu.roll(rows[time + 1, :, lanes], shift, 1)
            table[time, to, :] = jnp.where(keep, now, before)
            before = now
        return carry

    lax.fori_loop(0, TABLE, build, 0)

    level(0, tm, 4)
    level(1, tm_other, 2)
    level(0, tm, 5)
    level(1, tm_other, 3)
    level(0, tm, 6)

    half = PORTION * POLS * ROWS // 2
    x_rows = [wrap(a - x + NX, NX) * NZ * ROWS for a in range(NX)]

    def step(u, carry):
        k, part = u // 2, u % 2

        time = jnp.where(k < 2, y_hi, 1 - y_hi) * 2 + jnp.where(k % 2 == 0, core, 1 - core)
        first = part * half
        left = jnp.concatenate([
            table[time, pl.ds(pl.multiple_of(first + (PHASES - 1 - phase) * POLS * ROWS, 32), half), :]
            for phase in range(PHASES)
        ], 1)
        out = pl.ds(pl.multiple_of(first, half), half)
        right = jnp.concatenate([
            gathered[time, pl.ds(pl.multiple_of(row, 128), NZ * ROWS), :] for row in x_rows
        ], 0)
        d = lax.dot_general(left, right, (((1,), (1,)), ((), ())), preferred_element_type=jnp.float32)

        @pl.when(k == 0)
        def _():
            acc[out, :] = d

        @pl.when(k > 0)
        def _():
            acc[out, :] += d
        return carry

    lax.fori_loop(0, 1, step, 0)
    level(1, tm_other, 4)
    lax.fori_loop(1, 2, step, 0)
    planes(0, tm_partner)
    level(1, tm_other, 5)
    lax.fori_loop(2, 3, step, 0)
    level(1, tm_other, 6)
    lax.fori_loop(3, 6, step, 0)
    planes(1, tm_last)
    lax.fori_loop(6, 8, step, 0)
    for copy in sent:
        copy.wait_send()


def per_device(samples):
    m = PORTION * POLS * ROWS
    count = 2 * 68 + 7
    acc = pl.pallas_call(
        kernel_body,
        out_shape=jax.ShapeDtypeStruct((m, 512), jnp.float32),
        in_specs=[pl.BlockSpec(memory_space=pltpu.VMEM)],
        out_specs=pl.BlockSpec(memory_space=pltpu.VMEM),
        scratch_shapes=[
            pltpu.VMEM((TIMES, 512, BLOCK), jnp.bfloat16),
            pltpu.VMEM((TIMES + 1, POLS * ROWS, BLOCK), jnp.bfloat16),
            pltpu.VMEM((TIMES, TABLE * POLS * ROWS, 128), jnp.bfloat16),
            pltpu.VMEM((BLOCK, 128), jnp.float32),
            pltpu.SemaphoreType.DMA((count,)),
            pltpu.SemaphoreType.DMA((count,)),
        ],
        compiler_params=pltpu.CompilerParams(
            collective_id=0, has_side_effects=True, vmem_limit_bytes=40 * 2**20
        ),
        name="gather_correlate",
    )(samples.reshape(ROWS, BLOCK))
    scaled = acc * (1.0 / math.sqrt(BLOCK * TIMES))
    return scaled.reshape(PORTION, POLS, ROWS, 1, 512)


def solution(mesh):
    return jax.shard_map(
        per_device,
        mesh=mesh,
        in_specs=(P("antb", "anta", "tm"),),
        out_specs=P("tm", None, "anta", "antb", None),
        check_vma=False,
    )
```

```python
import math

import jax
import jax.numpy as jnp
from jax import lax
from jax.experimental import pallas as pl
from jax.experimental.pallas import tpu as pltpu
from jax.sharding import PartitionSpec as P

POLS = 2
ROWS = 16
BLOCK = 1536
PHASES = 12
TIMES = 4
NX, NZ, NY = 4, 8, 4
PORTION = 64
SCALE = 1.0 / math.sqrt(BLOCK * TIMES)
TABLE = PORTION + PHASES - 1
PAIR = POLS * ROWS
XS = (1, -1, 2)
CHUNKS = ((0, 4, 6), (6, 10, 12), (0, 3, 6))
ROUTES = {2: (0, 0, 0, 0), 3: (0, 0, 2, 2), 4: (0, 1, 2, 2)}
PLAN = (
    "bs", "a1", "b1", "y", "rows", "t0-75", "a2", "cs", "b2", "a3", "wa", "ma01", "c1", "b3", "ma12", "d1",
    "wb", "mb01", "c2", "d2", "mb12", "c3", "d3", "wc", "wd", "mcd02",
)


def halves(lanes):
    low, high = lanes
    middle = (low + high + 1) // 2
    return {1: (low, middle), -1: (middle, high)}


def kernel_body(x_ref, acc, gathered, rows, table, xt, send_sem, recv_sem):
    tm = lax.axis_index("tm")
    anta = lax.axis_index("anta")
    antb = lax.axis_index("antb")
    y_hi, core = tm // 2, tm % 2
    x, z = anta // NZ, anta % NZ
    y = y_hi * 2 + antb
    tm_partner = y_hi * 2 + (1 - core)
    tm_other = (1 - y_hi) * 2 + core
    tm_last = (1 - y_hi) * 2 + (1 - core)

    def wrap(value, size):
        return lax.rem(value + size, size)

    x_next = {s: wrap(x + s, NX) * NZ + z for s in XS}
    z_next = {s: x * NZ + wrap(z + s, NZ) for s in range(-3, 5)}
    z_row = {dz: wrap(z + dz, NZ) * ROWS for dz in range(-4, 5)}

    def at_x(s):
        return {"tm": tm, "anta": x_next[s], "antb": antb}

    def at_z(s):
        return {"tm": tm, "anta": z_next[s], "antb": antb}

    def at_y(s):
        there = wrap(y + s, NY)
        return {"tm": (there // 2) * 2 + core, "anta": anta, "antb": there % 2}

    partner = {"tm": tm_partner, "anta": anta, "antb": antb}
    opposite = {"tm": tm_other, "anta": anta, "antb": antb}

    arrivals, groups, sent = {}, {}, {}

    def copy_of(key, src, dst, device, group):
        n = arrivals.setdefault(key, len(arrivals))
        k = groups.setdefault(group, len(groups))
        return pltpu.make_async_remote_copy(
            src_ref=src, dst_ref=dst, send_sem=send_sem.at[k], recv_sem=recv_sem.at[n],
            device_id=device, device_id_type=pl.DeviceIdType.MESH,
        )

    def send(key, src, dst, device, group):
        copy = copy_of(key, src, dst, device, group)
        copy.start()
        sent[group] = sent.get(group, 0) + math.prod(src.shape) // (ROWS * 128)

    def drain():
        for group, units in sent.items():
            ref = units_of(units)
            copy_of("drain", ref, ref, partner, group).wait_send()

    def units_of(units):
        t, p, r, n = next(
            (t, p, r, n) for t in range(1, TIMES + 1) for p in range(1, NX + 1) for r in range(1, NZ + 1)
            for n in range(1, PHASES + 1) if t * p * r * n == units
        )
        return gathered.at[pl.ds(0, t), pl.ds(0, p), pl.ds(0, r * ROWS), pl.ds(0, n * 128)]

    def size(ref):
        return math.prod(ref.shape) // (ROWS * 128)

    def wait(key, dst):
        copy_of(key, dst, dst, partner, "drain").wait_recv()

    where, kept = {}, []

    def block(time, rx, dz, lanes):
        key = (rx, dz, lanes)
        row = pl.ds(pl.multiple_of(z_row[dz], ROWS), ROWS)
        lanes = pl.ds(lanes[0] * 128, (lanes[1] - lanes[0]) * 128)
        ref = gathered.at[time, rx if isinstance(rx, slice) else rx % NX, row, lanes]
        where[id(ref)] = key
        kept.append(ref)
        return ref

    def row_block(time, pol):
        return rows.at[time + 1, pl.ds(pl.multiple_of(pol * ROWS, ROWS), ROWS), :]

    aside = slice(1, NX)

    def gather_of(g, time, chunk, route, on_landed):
        low, cut, high = chunk
        whole, part_p, part_q = (low, high), (low, cut), (cut, high)
        source = (None,) + ROUTES[route]
        steps = {0: 0}
        for d in (1, 2, 3, 4):
            steps[d] = steps[source[d]] + 1

        def z_lanes(s, rx, d):
            lanes = whole if rx == 0 else part_q
            if d < 4:
                return lanes
            if source[4] == 0:
                return lanes if s == 1 else (high, high)
            return halves(lanes)[s]

        def send_z(s, rx, d):
            lanes = z_lanes(s, rx, d)
            if lanes[0] < lanes[1]:
                ref = block(time, rx, -s * source[d], lanes)
                send((g, steps[d] + (rx is aside), "z", s), ref, ref, at_z(s * (d - source[d])), (g, "z", rx is aside))

        def send_x(dz):
            lanes = whole if dz == 0 else part_p
            for s in XS:
                send((g, steps[abs(dz)] + 1, "x", s), block(time, 0, dz, lanes), block(time, -s, dz, lanes), at_x(s), (g, "x", dz == 0))

        def send_on(rx, s, at):
            for d in (1, 2, 3, 4):
                if source[d] == at:
                    send_z(s, rx, d)

        def wait_link(n, link, s, refs):
            wait((g, n, link, s), units_of(sum(size(ref) for ref in refs)))

        def z_refs(n, s):
            refs = []
            for rx, late in ((0, 0), (aside, 1)):
                for d in (1, 2, 3, 4):
                    lanes = z_lanes(s, rx, d)
                    if steps[d] + late == n and lanes[0] < lanes[1]:
                        refs.append(block(time, rx, -s * d, lanes))
            return refs

        def x_refs(n, s):
            return [
                block(time, -s, dz, part_p if dz else whole)
                for dz in (0, 1, -1, 2, -2, 3, -3, 4) if steps[abs(dz)] + 1 == n
            ]

        def start():
            for s in (1, -1):
                send_on(0, s, 0)
            send_x(0)
            on_landed(block(time, 0, 0, whole))

        def level(n):
            landed = []
            for s in (1, -1):
                refs = z_refs(n, s)
                if refs:
                    wait_link(n, "z", s, refs)
                    landed.extend(refs)
                for d in (1, 2, 3, 4):
                    if steps[d] == n:
                        send_on(0, s, d)
                    if steps[d] == n - 1:
                        send_on(aside, s, d)
                    if steps[d] == n and d < 4:
                        send_x(-s * d)
            if steps[4] == n:
                send_x(4)
            for s in XS:
                refs = x_refs(n, s)
                if refs:
                    wait_link(n, "x", s, refs)
                    landed.extend(refs)
            if n == 1:
                for s in (1, -1):
                    send_on(aside, s, 0)
            for ref in landed:
                on_landed(ref)
            if g == "b":
                marks.append(len(crossed))

        return start, level

    def to_core(g):
        def on_landed(ref):
            send((g, "core"), ref, ref, partner, (g, "core"))
        return on_landed

    crossed, marks = [], [0]

    def to_core_and_across(ref):
        send(("b", "core"), ref, ref, partner, ("b", "core"))
        if where[id(ref)][:2] != (0, 0):
            send(("d", len(marks)), ref, ref, opposite, ("d", "y", len(marks)))
            crossed.append(where[id(ref)])

    def landed_core(g):
        time, (low, _, high) = cores[g]
        wait((g, "core"), gathered.at[time, :, :, pl.ds(low * 128, (high - low) * 128)])

    gathers = {
        "a": gather_of("a", tm, CHUNKS[0], 3, to_core("a")),
        "b": gather_of("b", tm, CHUNKS[1], 3, to_core_and_across),
        "c": gather_of("c", tm_other, CHUNKS[2], 3, to_core("c")),
    }
    cores = {
        "a": (tm_partner, CHUNKS[0]), "b": (tm_partner, CHUNKS[1]),
        "c": (tm_last, CHUNKS[0]), "d": (tm_last, CHUNKS[1]),
    }

    def take_across(n):
        refs = [block(tm_other, *key) for key in crossed[marks[n - 1]:marks[n]]]
        wait(("d", n), units_of(sum(size(ref) for ref in refs)))
        for ref in refs:
            send(("d", "core"), ref, ref, partner, ("d", "core"))

    lane = lax.broadcasted_iota(jnp.int32, (PAIR, 128), 1)

    def build(n, carry):
        m = PHASES - 1 - n - PORTION * tm + PHASES * 32
        phase, shift = m % PHASES, 32 - m // PHASES
        lanes = pl.ds(pl.multiple_of(phase * 128, 128), 128)
        keep = lane >= shift
        to = pl.ds(pl.multiple_of(n * PAIR, PAIR), PAIR)
        before = pltpu.roll(rows[0, :, lanes], shift, 1)
        for time in range(TIMES):
            now = pltpu.roll(rows[time + 1, :, lanes], shift, 1)
            table[time, to, :] = jnp.where(keep, now, before)
            before = now
        return carry

    def build_part(low, high):
        lax.fori_loop(low, high, build, 0, unroll=5)

    half = PORTION * PAIR // 2
    planes = [wrap(a - x + NX, NX) for a in range(NX)]

    first_product, last_product = 'a', 'cd'

    def product(g):
        taken = [
            (time, cores[k][1][0], cores[k][1][2]) for k in g
            for time in ((tm, tm_partner) if k in "ab" else (tm_other, tm_last))
        ]

        def step(part, carry):
            first = part * half
            left = jnp.concatenate([
                table[time, pl.ds(pl.multiple_of(first + (PHASES - 1 - phase) * PAIR, PAIR), half), :]
                for time, low, high in taken for phase in range(low, high)
            ], 1)
            right = jnp.concatenate([
                jnp.concatenate([gathered[time, plane, :, pl.ds(low * 128, (high - low) * 128)] for time, low, high in taken], 1)
                for plane in planes
            ], 0)
            d = lax.dot_general(left, right, (((1,), (1,)), ((), ())), preferred_element_type=jnp.float32)
            for tile in range(4):
                to = pl.ds(4 * first + tile, half, stride=4)
                piece = d[:, tile * 128:(tile + 1) * 128]
                if g == first_product:
                    acc[to, :] = piece
                elif g != last_product:
                    acc[to, :] += piece
                else:
                    acc[to, :] = (acc[to, :] + piece) * SCALE
            return carry

        return step

    barrier = pltpu.get_barrier_semaphore()
    everyone = [at_x(s) for s in XS] + [at_z(s) for s in range(-3, 5) if s] + [at_y(1), at_y(-1), opposite, partner]
    for device in everyone:
        pl.semaphore_signal(barrier, inc=1, device_id=device, device_id_type=pl.DeviceIdType.MESH)
    own = x_ref[...].astype(jnp.float32)
    pad = jnp.zeros((128 - ROWS, 128), jnp.float32)
    for tile in range(PHASES):
        piece = jnp.concatenate([own[:, tile * 128:(tile + 1) * 128], pad], 0)
        xt[tile * 128:(tile + 1) * 128, :] = piece.T
    own_row = pl.multiple_of(z * ROWS, ROWS)
    pol_row = pl.multiple_of(antb * ROWS, ROWS)
    for phase in range(PHASES):
        piece = xt[pl.ds(phase, 128, stride=PHASES), :].T[:ROWS, :].astype(jnp.bfloat16)
        lanes = slice(phase * 128, (phase + 1) * 128)
        gathered[tm, 0, pl.ds(own_row, ROWS), lanes] = piece
        rows[tm + 1, pl.ds(pol_row, ROWS), lanes] = piece
    rows[0, :, :] = jnp.zeros((PAIR, BLOCK), jnp.bfloat16)
    pl.semaphore_wait(barrier, len(everyone))

    full = (0, PHASES)
    own_block = block(tm, 0, 0, full)

    def step_y():
        other_block = block(tm_other, 0, 0, full)
        wait("y2", other_block)
        send("other", other_block, row_block(tm_other, antb), partner, "rows")
        rows[tm_other + 1, pl.ds(pol_row, ROWS), :] = gathered[tm_other, 0, pl.ds(own_row, ROWS), :]
        for s in (1, -1):
            there = wrap(y - s, NY)
            ref = row_block((there // 2) * 2 + core, 1 - antb)
            wait(("y", s), ref)
            send(("row", s), ref, ref, partner, "rows")

    def start_c():
        gathers["c"][0]()
        d_own = block(tm_other, 0, 0, (CHUNKS[1][0], CHUNKS[1][2]))
        send(("d", "core"), d_own, d_own, partner, ("d", "core"))

    def step_rows():
        wait("own", row_block(tm_partner, antb))
        wait("other", row_block(tm_last, antb))
        for s in (1, -1):
            there = wrap(y - s, NY)
            wait(("row", s), row_block((there // 2) * 2 + 1 - core, 1 - antb))

    send("y2", own_block, own_block, opposite, "rows")
    for s in (1, -1):
        send(("y", s), own_block, row_block(tm, antb), at_y(s), "rows")
    gathers["a"][0]()
    send("own", own_block, row_block(tm, antb), partner, "rows")

    for word in PLAN:
        if word == "y":
            step_y()
        elif word == "cs":
            start_c()
        elif word == "bs":
            gathers["b"][0]()
        elif word == "rows":
            step_rows()
        elif word[0] == "t":
            low, high = word[1:].split("-")
            build_part(int(low), int(high))
        elif word[0] == "d":
            take_across(int(word[1]))
        elif word[0] == "w":
            landed_core(word[1])
        elif word[0] == "m":
            lax.fori_loop(int(word[-2]), int(word[-1]), product(word[1:-2]), 0)
        else:
            gathers[word[0]][1](int(word[1]))
    drain()


def per_device(samples):
    m = PORTION * PAIR
    acc = pl.pallas_call(
        kernel_body,
        out_shape=jax.ShapeDtypeStruct((m * 4, 128), jnp.float32),
        in_specs=[pl.BlockSpec(memory_space=pltpu.VMEM)],
        out_specs=pl.BlockSpec(memory_space=pltpu.VMEM),
        scratch_shapes=[
            pltpu.VMEM((TIMES, NX, NZ * ROWS, BLOCK), jnp.bfloat16),
            pltpu.VMEM((TIMES + 1, PAIR, BLOCK), jnp.bfloat16),
            pltpu.VMEM((TIMES, TABLE * PAIR, 128), jnp.bfloat16),
            pltpu.VMEM((BLOCK, 128), jnp.float32),
            pltpu.SemaphoreType.DMA((24,)),
            pltpu.SemaphoreType.DMA((64,)),
        ],
        compiler_params=pltpu.CompilerParams(
            collective_id=0, has_side_effects=True, vmem_limit_bytes=40 * 2**20
        ),
        name="gather_correlate",
    )(samples.reshape(ROWS, BLOCK))
    return acc.reshape(PORTION, POLS, ROWS, 1, 512)


def solution(mesh):
    return jax.shard_map(
        per_device,
        mesh=mesh,
        in_specs=(P("antb", "anta", "tm"),),
        out_specs=P("tm", None, "anta", "antb", None),
        check_vma=False,
    )
```
